32 devices in a mesh: dp: 8 (over y, x, core), mp: 4 (over z).
Axes of the slice: x: 2, y: 2, z: 4, core: 2. Of those that a mesh axis runs over, the one named last changes fastest.
Arguments:
- hidden: bfloat16 [64, 4096], P('dp'), may hold values from -6 to 6
- attention_gain: float32 [4096], replicated, may hold values from 0.5 to 1.5
- query_weight: bfloat16 [4096, 4096], P(None, 'mp'), may hold values from -0.09375 to 0.09375
- key_weight: bfloat16 [4096, 1024], P(None, 'mp'), may hold values from -0.09375 to 0.09375
- value_weight: bfloat16 [4096, 1024], P(None, 'mp'), may hold values from -0.09375 to 0.09375
- output_weight: bfloat16 [4096, 4096], P('mp'), may hold values from -0.09375 to 0.09375
- key_cache: bfloat16 [64, 8, 4096, 128], P('dp', 'mp'), may hold values from -9 to 9
- value_cache: bfloat16 [64, 8, 4096, 128], P('dp', 'mp'), may hold values from -8 to 8, as said below
- lengths: int32 [64], P('dp'), may hold values from 128 to 4096, as said below
- finished: int32 [64], P('dp'), may hold values 0 or 1
- feed_gain: float32 [4096], replicated, may hold values from 0.5 to 1.5
- gate_weight: bfloat16 [4096, 14336], P(None, ('dp', 'mp')), may hold values from -0.09375 to 0.09375
- up_weight: bfloat16 [4096, 14336], P(None, ('dp', 'mp')), may hold values from -0.09375 to 0.09375
- down_weight: bfloat16 [14336, 4096], P(('dp', 'mp')), may hold values from -0.046875 to 0.046875
- final_gain: float32 [4096], replicated, may hold values from 0.5 to 8, as said below
- vocab_weight: bfloat16 [4096, 128256], P(None, ('dp', 'mp')), may hold values from -0.375 to 0.375
- next_tokens: int32 [64], replicated, may hold values from 0 to 128255
Outputs:
- log_likelihood: float32 [64], P('dp')
The draws below stay inside these ranges and needn't reach their ends.
Inputs may be any that keep to these rules, and one draw needn't show every extreme that they name: `lengths`: each rollout has 128 to 4096 cached tokens; both ends are reached in every draw; rollouts held by one index of dp share a length scale, so devices' total cached tokens differ. `finished`: 0 or 1. `next_tokens`: a vocabulary entry. `value_cache`: a per-rollout and per-head mean plus noise. `final_gain`: positive gains.
All inputs are finite; a program needn't handle non-finite values.
Results may differ from the reference program's by a relative error of at most 0.0055.
Values may be sent and summed in bfloat16 or wider, within the bound.
A program may use at most 192 MiB of HBM per device.

```python
import math
import jax
import jax.numpy as jnp
from jax import lax

D = 4096
H = 32
KVH = 8
HD = 128
FF = 14336
VOCAB = 128256
ROLL_DEV = 8
MAXLEN = 4096
MINLEN = 128
ROLLOUTS = 64


def draw_value_cache(key, part):
    shape = (ROLLOUTS, KVH, MAXLEN, HD)
    center = jax.random.normal(jax.random.fold_in(key, 11), (ROLLOUTS, KVH, 1, HD), jnp.float32)
    center = jnp.clip(center, -3.0, 3.0)
    noise = jax.random.normal(jax.random.fold_in(key, 12), shape, jnp.float32)
    noise = jnp.clip(noise, -5.0, 5.0)
    return (center + noise).astype(jnp.bfloat16)


def draw_final_gain(key, part):
    gains = jax.random.uniform(jax.random.fold_in(key, 31), (D,), jnp.float32, 0.7, 1.3)
    return gains.astype(jnp.float32)


def draw_lengths(key, part):
    spread = MAXLEN - MINLEN + 1
    uniform_part = jax.random.randint(jax.random.fold_in(key, 21), (ROLLOUTS,), 0, spread)
    factor = jax.random.randint(jax.random.fold_in(key, 22), (ROLLOUTS // ROLL_DEV,), 1, 5)
    factor = jnp.repeat(factor * factor, ROLL_DEV)
    result = MINLEN + uniform_part * factor // 16
    longest = jax.random.randint(jax.random.fold_in(key, 23), (), 0, ROLLOUTS)
    shortest = (longest + 1 + jax.random.randint(jax.random.fold_in(key, 24), (), 0, ROLLOUTS - 1)) % ROLLOUTS
    places = jnp.arange(ROLLOUTS)
    result = jnp.where(places == longest, MAXLEN, result)
    result = jnp.where(places == shortest, MINLEN, result)
    return result.astype(jnp.int32)


def plant(values, rng, low, largest):
    dims = values.shape
    spot = [jax.random.randint(jax.random.fold_in(rng, axis), (), 0, dims[axis]) for axis in range(len(dims))]
    values = values.at[tuple(spot)].set(low)
    longest = dims.index(max(dims))
    spot[longest] = (spot[longest] + 1) % dims[longest]
    return values.at[tuple(spot)].set(largest)


def levels(key, shape, split, smallest, top_value):
    level = 1.0
    for dim, blocks in split:
        heights = jax.random.uniform(jax.random.fold_in(jax.random.fold_in(key, 6), dim), (blocks,), jnp.float32, smallest / len(split), top_value / len(split))
        level = level * jnp.repeat(jnp.exp(heights), shape[dim] // blocks).reshape((-1,) + (1,) * (len(shape) - 1 - dim))
    return level


def bell_draw(stream_key, dims, scale, limit, cuts=(), kind=jnp.bfloat16):
    entries = jax.random.normal(stream_key, dims, jnp.float32) * scale
    if len(cuts) > 0:
        entries = levels(stream_key, dims, cuts, -0.22, 0.18) * entries
    return jnp.clip(entries, min=-limit, max=limit).astype(kind)


def setup_inputs(seed: int = 0) -> dict:
    key_of = jax.random.split(jax.random.key(seed), 18)
    return {
        "hidden": bell_draw(key_of[0], (ROLLOUTS, D), 1.0, 6.0, ((0, 8),)),
        "attention_gain": jnp.clip(1.0 + 0.1 * jax.random.normal(key_of[1], (D,), jnp.float32), 0.5, 1.5),
        "query_weight": bell_draw(key_of[2], (D, H * HD), D ** -0.5, 0.09375, ((1, 4),)),
        "key_weight": bell_draw(key_of[3], (D, KVH * HD), D ** -0.5, 0.09375, ((1, 4),)),
        "value_weight": bell_draw(key_of[4], (D, KVH * HD), D ** -0.5, 0.09375, ((1, 4),)),
        "output_weight": bell_draw(key_of[5], (H * HD, D), (H * HD) ** -0.5, 0.09375, ((0, 4),)),
        "key_cache": bell_draw(key_of[6], (ROLLOUTS, KVH, MAXLEN, HD), 1.5, 9.0, ((0, 8), (1, 4))),
        "value_cache": draw_value_cache(jax.random.fold_in(key_of[17], 71), 0),
        "lengths": draw_lengths(jax.random.fold_in(key_of[17], 71), 0),
        "finished": plant((jax.random.randint(key_of[9], (ROLLOUTS,), 0, 8) < 1).astype(jnp.int32), jax.random.fold_in(key_of[9], 1), 0, 1),
        "feed_gain": jnp.clip(1.0 + 0.1 * jax.random.normal(key_of[10], (D,), jnp.float32), 0.5, 1.5),
        "gate_weight": bell_draw(key_of[11], (D, FF), D ** -0.5, 0.09375, ((1, 32),)),
        "up_weight": bell_draw(key_of[12], (D, FF), D ** -0.5, 0.09375, ((1, 32),)),
        "down_weight": bell_draw(key_of[13], (FF, D), FF ** -0.5, 0.046875, ((0, 32),)),
        "final_gain": draw_final_gain(jax.random.fold_in(key_of[17], 71), 0),
        "vocab_weight": bell_draw(key_of[15], (D, VOCAB), (D // 16) ** -0.5, 0.375, ((1, 32),)),
        "next_tokens": plant(jax.random.randint(key_of[16], (ROLLOUTS,), 0, VOCAB), jax.random.fold_in(key_of[16], 1), 0, VOCAB - 1).astype(jnp.int32),
    }


EPSILON = 1e-05
THETA = 500000.0
NEGATIVE = -1e+30

def rms_norm(hidden, gain):
    wide = hidden.astype(jnp.float32)
    scale = lax.rsqrt(lax.optimization_barrier(jnp.mean(wide * wide, axis=-1, keepdims=True)) + EPSILON)
    return (wide * scale * gain).astype(jnp.bfloat16)

def rotate(heads, positions):
    half = heads.shape[-1] // 2
    exponent = jnp.arange(half, dtype=jnp.float32) * (-2.0 / heads.shape[-1])
    frequency = jnp.power(jnp.float32(THETA), exponent)
    angles = positions.astype(jnp.float32)[:, None, None] * frequency[None, None, :]
    cosine = jnp.cos(angles)
    sine = jnp.sin(angles)
    former = heads[..., :half]
    latter = heads[..., half:]
    return jnp.concatenate([former * cosine - latter * sine, latter * cosine + former * sine], axis=-1)

def attend_one(inputs):
    query, keys, values, own_key, own_value, length = inputs
    scale = 1.0 / math.sqrt(query.shape[-1])
    scores = jnp.einsum('kgd,kld->kgl', query.astype(jnp.float32), keys.astype(jnp.float32)) * scale
    places = jnp.arange(keys.shape[1], dtype=jnp.int32)
    scores = jnp.where(places[None, None, :] < length, scores, NEGATIVE)
    own = jnp.einsum('kgd,kd->kg', query.astype(jnp.float32), own_key.astype(jnp.float32)) * scale
    top = jnp.maximum(lax.optimization_barrier(jnp.max(scores, axis=-1)), own)
    weights = jnp.exp(scores - top[..., None])
    own_weight = jnp.exp(own - top)
    total = lax.optimization_barrier(jnp.sum(weights, axis=-1)) + own_weight
    rounded = lax.optimization_barrier(weights.astype(jnp.bfloat16)).astype(jnp.float32)
    mixed = jnp.einsum('kgl,kld->kgd', rounded, values.astype(jnp.float32))
    mixed = mixed + own_weight[..., None] * own_value.astype(jnp.float32)[:, None, :]
    return (mixed / total[..., None]).astype(jnp.bfloat16)

def reference(hidden, attention_gain, query_weight, key_weight, value_weight, output_weight, key_cache, value_cache, lengths, finished, feed_gain, gate_weight, up_weight, down_weight, final_gain, vocab_weight, next_tokens):
    rollouts = hidden.shape[0]
    groups = H // KVH
    normed = rms_norm(hidden, attention_gain)
    queries = jnp.dot(normed, query_weight, preferred_element_type=jnp.float32).reshape(rollouts, H, HD)
    queries = rotate(queries, lengths).astype(jnp.bfloat16).reshape(rollouts, KVH, groups, HD)
    new_keys = jnp.dot(normed, key_weight, preferred_element_type=jnp.float32).reshape(rollouts, KVH, HD)
    new_keys = rotate(new_keys, lengths).astype(jnp.bfloat16)
    new_values = jnp.dot(normed, value_weight, preferred_element_type=jnp.float32).astype(jnp.bfloat16).reshape(rollouts, KVH, HD)
    attended = lax.map(attend_one, (queries, key_cache, value_cache, new_keys, new_values, lengths.astype(jnp.int32)))
    attention = jnp.dot(attended.reshape(rollouts, H * HD), output_weight, preferred_element_type=jnp.float32)
    mixed_hidden = (hidden.astype(jnp.float32) + attention).astype(jnp.bfloat16)
    feed_in = rms_norm(mixed_hidden, feed_gain)
    gate = jnp.dot(feed_in, gate_weight, preferred_element_type=jnp.float32)
    upward = jnp.dot(feed_in, up_weight, preferred_element_type=jnp.float32)
    activation = (jax.nn.silu(gate) * upward).astype(jnp.bfloat16)
    feed = jnp.dot(activation, down_weight, preferred_element_type=jnp.float32)
    residual = (mixed_hidden.astype(jnp.float32) + feed).astype(jnp.bfloat16)
    final = rms_norm(residual, final_gain)
    logits = jnp.dot(final, vocab_weight, preferred_element_type=jnp.float32)
    top = lax.optimization_barrier(jnp.max(logits, axis=-1))
    normalizer = top + jnp.log(lax.optimization_barrier(jnp.sum(jnp.exp(logits - top[:, None]), axis=-1)))
    picked = jnp.take_along_axis(logits, next_tokens.astype(jnp.int32)[:, None], axis=1)[:, 0]
    return jnp.where(finished != 0, 0.0, picked - normalizer).astype(jnp.float32)
```

```python
import functools
import math

import jax
import jax.numpy as jnp
from jax import lax
from jax.experimental import pallas as pl
from jax.experimental.pallas import tpu as pltpu
from jax.sharding import PartitionSpec as P

H = 32
KVH = 8


EPSILON = 1e-05
THETA = 500000.0
NEGATIVE = -1e30


def rms_norm(hidden, gain):
    wide = hidden.astype(jnp.float32)
    scale = lax.rsqrt(jnp.mean(wide * wide, axis=-1, keepdims=True) + EPSILON)
    return (wide * scale * gain).astype(jnp.bfloat16)


def rotate(heads, positions):
    half = heads.shape[-1] // 2
    exponent = jnp.arange(half, dtype=jnp.float32) * (-2.0 / heads.shape[-1])
    frequency = jnp.power(jnp.float32(THETA), exponent)
    angles = positions.astype(jnp.float32)[:, None, None] * frequency[None, None, :]
    cosine = jnp.cos(angles)
    sine = jnp.sin(angles)
    former = heads[..., :half]
    latter = heads[..., half:]
    return jnp.concatenate(
        [former * cosine - latter * sine, latter * cosine + former * sine], axis=-1
    )


MESH = pl.DeviceIdType.MESH
VMEM = pltpu.VMEM


def greet(n_dp, n_mp):
    dp, mp = lax.axis_index("dp"), lax.axis_index("mp")
    barrier = pltpu.get_barrier_semaphore()
    for step in range(1, n_mp):
        pl.semaphore_signal(
            barrier, inc=1, device_id=(dp, lax.rem(mp + step, n_mp)), device_id_type=MESH
        )
    for step in range(1, n_dp):
        pl.semaphore_signal(
            barrier, inc=1, device_id=(lax.rem(dp + step, n_dp), mp), device_id_type=MESH
        )
    pl.semaphore_wait(barrier, n_mp + n_dp - 2)
    return dp, mp


def exchange(sources, targets, sends, receives, peers):
    copies = []
    for step, (source, target, peer) in enumerate(zip(sources, targets, peers)):
        copy = pltpu.make_async_remote_copy(
            src_ref=source,
            dst_ref=target,
            send_sem=sends.at[step],
            recv_sem=receives.at[step],
            device_id=peer,
            device_id_type=MESH,
        )
        copy.start()
        copies.append(copy)
    return copies


def across_mp(dp, mp, n_mp):
    return [(dp, lax.rem(mp + step, n_mp)) for step in range(1, n_mp)]


def across_dp(dp, mp, n_dp):
    return [(lax.rem(dp + step, n_dp), mp) for step in range(1, n_dp)]


def normalized(wide, gain):
    scale = lax.rsqrt(jnp.mean(wide * wide, axis=-1, keepdims=True) + EPSILON)
    return (wide * scale * gain).astype(jnp.bfloat16)


def spread_rows(gathered_ref, dp, mp, n_dp, sends, receives):
    mine = gathered_ref.at[dp]
    copies = exchange(
        [mine] * (n_dp - 1),
        [mine] * (n_dp - 1),
        sends,
        receives,
        across_dp(dp, mp, n_dp),
    )
    for copy in copies:
        copy.wait()


def after_attention(
    n_dp, n_mp, partial_ref, hidden_ref, gain_ref, gathered_ref, mixed_ref,
    landed, mp_send, mp_receive, dp_send, dp_receive,
):
    dp, mp = greet(n_dp, n_mp)
    copies = exchange(
        [partial_ref] * (n_mp - 1),
        [landed.at[step] for step in range(n_mp - 1)],
        mp_send,
        mp_receive,
        across_mp(dp, mp, n_mp),
    )
    total = partial_ref[...].astype(jnp.float32)
    for step, copy in enumerate(copies):
        copy.wait()
        total = total + landed[step].astype(jnp.float32)
    mixed = (hidden_ref[...].astype(jnp.float32) + total).astype(jnp.bfloat16)
    mixed_ref[...] = mixed
    gathered_ref[dp] = normalized(mixed.astype(jnp.float32), gain_ref[...])
    spread_rows(gathered_ref, dp, mp, n_dp, dp_send, dp_receive)


def after_feed(
    n_dp, n_mp, partial_ref, mixed_ref, gain_ref, gathered_ref,
    arrived, summed, landed, rs_send, rs_receive, mp_send, mp_receive, dp_send, dp_receive,
):
    dp, mp = greet(n_dp, n_mp)
    copies = exchange(
        [partial_ref.at[lax.rem(dp + step, n_dp)] for step in range(1, n_dp)],
        [arrived.at[step] for step in range(n_dp - 1)],
        rs_send,
        rs_receive,
        across_dp(dp, mp, n_dp),
    )
    total = partial_ref[dp].astype(jnp.float32)
    for step, copy in enumerate(copies):
        copy.wait()
        total = total + arrived[step].astype(jnp.float32)
    summed[...] = total.astype(jnp.bfloat16)
    copies = exchange(
        [summed] * (n_mp - 1),
        [landed.at[step] for step in range(n_mp - 1)],
        mp_send,
        mp_receive,
        across_mp(dp, mp, n_mp),
    )
    total = summed[...].astype(jnp.float32)
    for step, copy in enumerate(copies):
        copy.wait()
        total = total + landed[step].astype(jnp.float32)
    residual = (mixed_ref[...].astype(jnp.float32) + total).astype(jnp.bfloat16)
    gathered_ref[dp] = normalized(residual.astype(jnp.float32), gain_ref[...])
    spread_rows(gathered_ref, dp, mp, n_dp, dp_send, dp_receive)


def joined_stats(pieces):
    highest = pieces[0][0:1]
    for piece in pieces[1:]:
        highest = jnp.maximum(highest, piece[0:1])
    spread = sum(piece[1:2] * jnp.exp(piece[0:1] - highest) for piece in pieces)
    picked = sum(piece[2:3] for piece in pieces)
    return highest, spread, picked


def after_logits(
    n_dp, n_mp, stats_ref, out_ref,
    landed, joint, arrived, mp_send, mp_receive, dp_send, dp_receive,
):
    dp, mp = greet(n_dp, n_mp)
    copies = exchange(
        [stats_ref] * (n_mp - 1),
        [landed.at[step] for step in range(n_mp - 1)],
        mp_send,
        mp_receive,
        across_mp(dp, mp, n_mp),
    )
    for copy in copies:
        copy.wait()
    highest, spread, picked = joined_stats(
        [stats_ref[...]] + [landed[step] for step in range(n_mp - 1)]
    )
    joint[...] = jnp.zeros_like(joint)
    joint[0:1] = highest
    joint[1:2] = spread
    joint[2:3] = picked
    copies = exchange(
        [joint] * (n_dp - 1),
        [arrived.at[step] for step in range(n_dp - 1)],
        dp_send,
        dp_receive,
        across_dp(dp, mp, n_dp),
    )
    for copy in copies:
        copy.wait()
    highest, spread, picked = joined_stats(
        [joint[...]] + [arrived[step] for step in range(n_dp - 1)]
    )
    result = picked - (highest + jnp.log(spread))
    out_ref[...] = jnp.broadcast_to(result, out_ref.shape)


def pairs(count):
    return [pltpu.SemaphoreType.DMA((max(count, 1),))] * 2


def comm_call(kernel, operands, out_shape, scratch, number):
    return pl.pallas_call(
        kernel,
        out_shape=out_shape,
        in_specs=[pl.BlockSpec(memory_space=VMEM)] * len(operands),
        out_specs=jax.tree.map(lambda _: pl.BlockSpec(memory_space=VMEM), out_shape),
        scratch_shapes=scratch,
        compiler_params=pltpu.CompilerParams(
            collective_id=number, has_side_effects=True, vmem_limit_bytes=8 * 1024 * 1024
        ),
    )(*operands)


def padded_attention(queries, own, key_cache, value_cache, new_values, lengths):
    head_width = queries.shape[-1]
    scale = 1.0 / math.sqrt(head_width)
    scores = (
        jnp.einsum("rkgd,rkld->rkgl", queries, key_cache, preferred_element_type=jnp.float32)
        * scale
    )
    places = lax.broadcasted_iota(jnp.int32, (1, 1, 1, key_cache.shape[2]), 3)
    scores = jnp.where(places < lengths[:, None, None, None], scores, NEGATIVE)
    top = jnp.maximum(jnp.max(scores, axis=-1), own)
    weights = jnp.exp(scores - top[..., None])
    own_weight = jnp.exp(own - top)
    total = jnp.sum(weights, axis=-1) + own_weight
    mixed = jnp.einsum(
        "rkgl,rkld->rkgd",
        weights.astype(jnp.bfloat16),
        value_cache,
        preferred_element_type=jnp.float32,
    )
    mixed = mixed + own_weight[..., None] * new_values.astype(jnp.float32)[:, :, None, :]
    return (mixed / total[..., None]).astype(jnp.bfloat16)


def shards(
    hidden,
    attention_gain,
    query_weight,
    key_weight,
    value_weight,
    output_weight,
    key_cache,
    value_cache,
    lengths,
    finished,
    feed_gain,
    gate_weight,
    up_weight,
    down_weight,
    final_gain,
    vocab_weight,
    next_tokens,
):
    local_rows = hidden.shape[0]
    key_heads = key_cache.shape[1]
    head_width = key_cache.shape[3]
    groups = H // KVH
    normed = rms_norm(hidden, attention_gain)
    queries = jnp.dot(normed, query_weight, preferred_element_type=jnp.float32).reshape(
        local_rows, key_heads * groups, head_width
    )
    queries = (
        rotate(queries, lengths)
        .astype(jnp.bfloat16)
        .reshape(local_rows, key_heads, groups, head_width)
    )
    new_keys = jnp.dot(normed, key_weight, preferred_element_type=jnp.float32).reshape(
        local_rows, key_heads, head_width
    )
    new_keys = rotate(new_keys, lengths).astype(jnp.bfloat16)
    new_values = (
        jnp.dot(normed, value_weight, preferred_element_type=jnp.float32)
        .astype(jnp.bfloat16)
        .reshape(local_rows, key_heads, head_width)
    )
    own = jnp.einsum("rkgd,rkd->rkg", queries, new_keys, preferred_element_type=jnp.float32) * (
        1.0 / math.sqrt(head_width)
    )
    attended = padded_attention(queries, own, key_cache, value_cache, new_values, lengths)
    partial_heads = jnp.dot(
        attended.reshape(local_rows, key_heads * groups * head_width),
        output_weight,
        preferred_element_type=jnp.float32,
    )
    n_dp, n_mp = lax.axis_size("dp"), lax.axis_size("mp")
    width = hidden.shape[1]
    row_type = jax.ShapeDtypeStruct((local_rows, width), jnp.bfloat16)
    all_rows = jax.ShapeDtypeStruct((n_dp, local_rows, width), jnp.bfloat16)
    landing = VMEM((max(n_mp - 1, 1), local_rows, width), jnp.bfloat16)
    feed_in, mixed_hidden = comm_call(
        functools.partial(after_attention, n_dp, n_mp),
        (partial_heads.astype(jnp.bfloat16), hidden, feed_gain[None]),
        (all_rows, row_type),
        [landing] + pairs(n_mp - 1) + pairs(n_dp - 1),
        1,
    )
    feed_in = feed_in.reshape(n_dp * local_rows, width)
    gate = jnp.dot(feed_in, gate_weight, preferred_element_type=jnp.float32)
    upward = jnp.dot(feed_in, up_weight, preferred_element_type=jnp.float32)
    activation = (jax.nn.silu(gate) * upward).astype(jnp.bfloat16)
    partial_feed = jnp.dot(activation, down_weight, preferred_element_type=jnp.float32)
    final = comm_call(
        functools.partial(after_feed, n_dp, n_mp),
        (
            partial_feed.astype(jnp.bfloat16).reshape(n_dp, local_rows, width),
            mixed_hidden,
            final_gain[None],
        ),
        all_rows,
        [
            VMEM((n_dp - 1, local_rows, width), jnp.bfloat16),
            VMEM((local_rows, width), jnp.bfloat16),
            landing,
        ]
        + pairs(n_dp - 1)
        + pairs(n_mp - 1)
        + pairs(n_dp - 1),
        2,
    )
    final = final.reshape(n_dp * local_rows, width)
    logits = jnp.dot(final, vocab_weight, preferred_element_type=jnp.float32)
    vocab_local = vocab_weight.shape[1]
    vocab_start = (lax.axis_index("dp") * n_mp + lax.axis_index("mp")) * vocab_local
    offsets = next_tokens - vocab_start
    matches = lax.broadcasted_iota(jnp.int32, (1, vocab_local), 1) == offsets[:, None]
    picked = jnp.sum(jnp.where(matches, logits, 0.0), axis=-1)
    local_top = jnp.max(logits, axis=-1)
    local_spread = jnp.sum(jnp.exp(logits - local_top[:, None]), axis=-1)
    rollouts = next_tokens.shape[0]
    lanes = -(-rollouts // 128) * 128
    stats = jnp.pad(
        jnp.stack([local_top, local_spread, picked]), ((0, 5), (0, lanes - rollouts))
    )
    chosen = comm_call(
        functools.partial(after_logits, n_dp, n_mp),
        (stats,),
        jax.ShapeDtypeStruct((8, lanes), jnp.float32),
        [
            VMEM((max(n_mp - 1, 1), 8, lanes), jnp.float32),
            VMEM((8, lanes), jnp.float32),
            VMEM((n_dp - 1, 8, lanes), jnp.float32),
        ]
        + pairs(n_mp - 1)
        + pairs(n_dp - 1),
        3,
    )
    chosen = lax.dynamic_slice_in_dim(chosen[0], lax.axis_index("dp") * local_rows, local_rows, 0)
    return jnp.where(finished != 0, 0.0, chosen).astype(jnp.float32)


def solution(mesh):
    in_specs = (
        P("dp", None),
        P(),
        P(None, "mp"),
        P(None, "mp"),
        P(None, "mp"),
        P("mp", None),
        P("dp", "mp", None, None),
        P("dp", "mp", None, None),
        P("dp"),
        P("dp"),
        P(),
        P(None, ("dp", "mp")),
        P(None, ("dp", "mp")),
        P(("dp", "mp"), None),
        P(),
        P(None, ("dp", "mp")),
        P(),
    )
    out_specs = P("dp")
    return jax.shard_map(shards, mesh=mesh, in_specs=in_specs, out_specs=out_specs, check_vma=False)
```

```python
import functools
import math

import jax
import jax.numpy as jnp
from jax import lax
from jax.experimental import pallas as pl
from jax.experimental.pallas import tpu as pltpu
from jax.sharding import PartitionSpec as P

H = 32
KVH = 8


EPSILON = 1e-05
THETA = 500000.0
NEGATIVE = -1e30


def rms_norm(hidden, gain):
    wide = hidden.astype(jnp.float32)
    scale = lax.rsqrt(jnp.mean(wide * wide, axis=-1, keepdims=True) + EPSILON)
    return (wide * scale * gain).astype(jnp.bfloat16)


def rotate(heads, positions):
    half = heads.shape[-1] // 2
    exponent = jnp.arange(half, dtype=jnp.float32) * (-2.0 / heads.shape[-1])
    frequency = jnp.power(jnp.float32(THETA), exponent)
    angles = positions.astype(jnp.float32)[:, None, None] * frequency[None, None, :]
    cosine = jnp.cos(angles)
    sine = jnp.sin(angles)
    former = heads[..., :half]
    latter = heads[..., half:]
    return jnp.concatenate(
        [former * cosine - latter * sine, latter * cosine + former * sine], axis=-1
    )


MESH = pl.DeviceIdType.MESH
VMEM = pltpu.VMEM


def greet(n_dp, n_mp):
    dp, mp = lax.axis_index("dp"), lax.axis_index("mp")
    barrier = pltpu.get_barrier_semaphore()
    for step in range(1, n_mp):
        pl.semaphore_signal(
            barrier, inc=1, device_id=(dp, lax.rem(mp + step, n_mp)), device_id_type=MESH
        )
    for step in range(1, n_dp):
        pl.semaphore_signal(
            barrier, inc=1, device_id=(lax.rem(dp + step, n_dp), mp), device_id_type=MESH
        )
    pl.semaphore_wait(barrier, n_mp + n_dp - 2)
    return dp, mp


def exchange(sources, targets, sends, receives, peers):
    copies = []
    for step, (source, target, peer) in enumerate(zip(sources, targets, peers)):
        copy = pltpu.make_async_remote_copy(
            src_ref=source,
            dst_ref=target,
            send_sem=sends.at[step],
            recv_sem=receives.at[step],
            device_id=peer,
            device_id_type=MESH,
        )
        copy.start()
        copies.append(copy)
    return copies


def across_mp(dp, mp, n_mp):
    return [(dp, lax.rem(mp + step, n_mp)) for step in range(1, n_mp)]


def across_dp(dp, mp, n_dp):
    return [(lax.rem(dp + step, n_dp), mp) for step in range(1, n_dp)]


def normalized(wide, gain):
    scale = lax.rsqrt(jnp.mean(wide * wide, axis=-1, keepdims=True) + EPSILON)
    return (wide * scale * gain).astype(jnp.bfloat16)


def spread_rows(gathered_ref, dp, mp, n_dp, sends, receives):
    mine = gathered_ref.at[dp]
    if n_dp % 2 == 1 or n_dp == 2:
        copies = exchange(
            [mine] * (n_dp - 1),
            [mine] * (n_dp - 1),
            sends,
            receives,
            across_dp(dp, mp, n_dp),
        )
        for copy in copies:
            copy.wait()
        return
    half = n_dp // 2
    twin = (dp + 1 - 2 * lax.rem(dp, 2), mp)
    peers = [(lax.rem(dp + 2 * step, n_dp), mp) for step in range(1, half)]
    copies = exchange([mine] * half, [mine] * half, sends, receives, peers + [twin])
    for step in range(1, half):
        copies[step - 1].wait_recv()
        rows = gathered_ref.at[lax.rem(dp - 2 * step + n_dp, n_dp)]
        forward = pltpu.make_async_remote_copy(
            src_ref=rows,
            dst_ref=rows,
            send_sem=sends.at[half - 1 + step],
            recv_sem=receives.at[half - 1 + step],
            device_id=twin,
            device_id_type=MESH,
        )
        forward.start()
        copies.append(forward)
    for place, copy in enumerate(copies):
        copy.wait_send()
        if place >= half - 1:
            copy.wait_recv()


def after_attention(
    n_dp, n_mp, partial_ref, hidden_ref, gain_ref, gathered_ref, mixed_ref,
    landed, mp_send, mp_receive, dp_send, dp_receive,
):
    dp, mp = greet(n_dp, n_mp)
    copies = exchange(
        [partial_ref] * (n_mp - 1),
        [landed.at[step] for step in range(n_mp - 1)],
        mp_send,
        mp_receive,
        across_mp(dp, mp, n_mp),
    )
    total = partial_ref[...].astype(jnp.float32)
    for step, copy in enumerate(copies):
        copy.wait()
        total = total + landed[step].astype(jnp.float32)
    mixed = (hidden_ref[...].astype(jnp.float32) + total).astype(jnp.bfloat16)
    mixed_ref[...] = mixed
    gathered_ref[dp] = normalized(mixed.astype(jnp.float32), gain_ref[...])
    spread_rows(gathered_ref, dp, mp, n_dp, dp_send, dp_receive)


def after_feed(
    n_dp, n_mp, partial_ref, mixed_ref, gain_ref, gathered_ref,
    arrived, summed, landed, rs_send, rs_receive, mp_send, mp_receive, dp_send, dp_receive,
):
    dp, mp = greet(n_dp, n_mp)
    copies = exchange(
        [partial_ref.at[lax.rem(dp + step, n_dp)] for step in range(1, n_dp)],
        [arrived.at[step] for step in range(n_dp - 1)],
        rs_send,
        rs_receive,
        across_dp(dp, mp, n_dp),
    )
    total = partial_ref[dp].astype(jnp.float32)
    for step, copy in enumerate(copies):
        copy.wait()
        total = total + arrived[step].astype(jnp.float32)
    summed[...] = total.astype(jnp.bfloat16)
    copies = exchange(
        [summed] * (n_mp - 1),
        [landed.at[step] for step in range(n_mp - 1)],
        mp_send,
        mp_receive,
        across_mp(dp, mp, n_mp),
    )
    total = summed[...].astype(jnp.float32)
    for step, copy in enumerate(copies):
        copy.wait()
        total = total + landed[step].astype(jnp.float32)
    residual = (mixed_ref[...].astype(jnp.float32) + total).astype(jnp.bfloat16)
    gathered_ref[dp] = normalized(residual.astype(jnp.float32), gain_ref[...])
    spread_rows(gathered_ref, dp, mp, n_dp, dp_send, dp_receive)


def joined_stats(pieces):
    highest = pieces[0][0:1]
    for piece in pieces[1:]:
        highest = jnp.maximum(highest, piece[0:1])
    spread = sum(piece[1:2] * jnp.exp(piece[0:1] - highest) for piece in pieces)
    picked = sum(piece[2:3] for piece in pieces)
    return highest, spread, picked


def after_logits(
    n_dp, n_mp, stats_ref, out_ref,
    landed, joint, arrived, mp_send, mp_receive, dp_send, dp_receive,
):
    dp, mp = greet(n_dp, n_mp)
    copies = exchange(
        [stats_ref] * (n_mp - 1),
        [landed.at[step] for step in range(n_mp - 1)],
        mp_send,
        mp_receive,
        across_mp(dp, mp, n_mp),
    )
    for copy in copies:
        copy.wait()
    highest, spread, picked = joined_stats(
        [stats_ref[...]] + [landed[step] for step in range(n_mp - 1)]
    )
    joint[...] = jnp.zeros_like(joint)
    joint[0:1] = highest
    joint[1:2] = spread
    joint[2:3] = picked
    copies = exchange(
        [joint] * (n_dp - 1),
        [arrived.at[step] for step in range(n_dp - 1)],
        dp_send,
        dp_receive,
        across_dp(dp, mp, n_dp),
    )
    for copy in copies:
        copy.wait()
    highest, spread, picked = joined_stats(
        [joint[...]] + [arrived[step] for step in range(n_dp - 1)]
    )
    result = picked - (highest + jnp.log(spread))
    out_ref[...] = jnp.broadcast_to(result, out_ref.shape)


def pairs(count):
    return [pltpu.SemaphoreType.DMA((max(count, 1),))] * 2


def comm_call(kernel, operands, out_shape, scratch, number):
    return pl.pallas_call(
        kernel,
        out_shape=out_shape,
        in_specs=[pl.BlockSpec(memory_space=VMEM)] * len(operands),
        out_specs=jax.tree.map(lambda _: pl.BlockSpec(memory_space=VMEM), out_shape),
        scratch_shapes=scratch,
        compiler_params=pltpu.CompilerParams(
            collective_id=number, has_side_effects=True, vmem_limit_bytes=8 * 1024 * 1024
        ),
    )(*operands)


def ragged_attention(
    block, lengths_ref, query_ref, key_ref, value_ref, key_hbm, value_hbm, out_ref,
    keys, values, key_sem, value_sem, tops, totals, sums,
):
    rollouts, heads, width = query_ref.shape
    key_heads = key_ref.shape[1]
    groups = heads // key_heads
    depth = keys.shape[0]
    scale = 1.0 / math.sqrt(width)
    owner = lax.broadcasted_iota(jnp.int32, (heads, 1), 0) // groups

    def by_head(pieces):
        joint = pieces[0]
        for head in range(1, key_heads):
            joint = jnp.where(owner == head, pieces[head], joint)
        return joint

    def blocks_of(row):
        return lax.div(lengths_ref[jnp.minimum(row, rollouts - 1)] + (block - 1), block)

    def following(row, part):
        last = part + 1 >= blocks_of(row)
        return jnp.where(last, row + 1, row), jnp.where(last, 0, part + 1)

    def copies(slot, row, part):
        places = pl.ds(pl.multiple_of(part * block, block), block)
        return (
            pltpu.make_async_copy(
                key_hbm.at[row, :, places, :], keys.at[slot], key_sem.at[slot]
            ),
            pltpu.make_async_copy(
                value_hbm.at[row, :, places, :], values.at[slot], value_sem.at[slot]
            ),
        )

    def fetch(slot, row, part):
        for copy in copies(slot, row, part):
            copy.start()

    steps = sum(blocks_of(row) for row in range(rollouts))
    ahead = (jnp.int32(0), jnp.int32(0))
    for slot in range(depth - 1):
        def begin(slot=slot, ahead=ahead):
            fetch(slot, *ahead)

        pl.when(slot < steps)(begin)
        ahead = following(*ahead)

    def step_body(step, carry):
        row, part, ahead_row, ahead_part = carry
        slot = lax.rem(step, depth)

        @pl.when(step + (depth - 1) < steps)
        def _():
            fetch(lax.rem(step + (depth - 1), depth), ahead_row, ahead_part)

        query = query_ref[row]

        @pl.when(part == 0)
        def _():
            own_key = by_head([key_ref[row, head : head + 1] for head in range(key_heads)])
            own_value = by_head([value_ref[row, head : head + 1] for head in range(key_heads)])
            own = jnp.sum(query * own_key, axis=-1, keepdims=True) * scale
            tops[...] = jnp.broadcast_to(own, tops.shape)
            totals[...] = jnp.ones_like(totals)
            sums[...] = jnp.broadcast_to(own_value, sums.shape)

        key_copy, value_copy = copies(slot, row, part)
        key_copy.wait()
        narrow = query.astype(jnp.bfloat16)
        scores = by_head(
            [
                lax.dot_general(
                    narrow,
                    keys[slot, head],
                    (((1,), (1,)), ((), ())),
                    preferred_element_type=jnp.float32,
                )
                for head in range(key_heads)
            ]
        )
        places = part * block + lax.broadcasted_iota(jnp.int32, (1, block), 1)
        scores = jnp.where(places < lengths_ref[row], scores * scale, NEGATIVE)
        former = tops[:, 0:1]
        top = jnp.maximum(former, jnp.max(scores, axis=-1, keepdims=True))
        fade = jnp.exp(former - top)
        weights = jnp.exp(scores - top)
        total = totals[:, 0:1] * fade + jnp.sum(weights, axis=-1, keepdims=True)
        rounded = weights.astype(jnp.bfloat16)
        value_copy.wait()
        mixed = by_head(
            [
                jnp.dot(rounded, values[slot, head], preferred_element_type=jnp.float32)
                for head in range(key_heads)
            ]
        )
        mixed = sums[...] * fade + mixed
        tops[...] = jnp.broadcast_to(top, tops.shape)
        totals[...] = jnp.broadcast_to(total, totals.shape)
        sums[...] = mixed
        out_ref[row] = (mixed / total).astype(jnp.bfloat16)
        return following(row, part) + following(ahead_row, ahead_part)

    lax.fori_loop(0, steps, step_body, (jnp.int32(0), jnp.int32(0)) + ahead)


def cached_attention(queries, new_keys, new_values, key_cache, value_cache, lengths):
    rollouts, key_heads, places, width = key_cache.shape
    heads = queries.shape[1]
    block = math.gcd(places, 2048)
    buffers = VMEM((3, key_heads, block, width), jnp.bfloat16)
    whole = pl.BlockSpec(memory_space=VMEM)
    away = pl.BlockSpec(memory_space=pl.ANY)
    return pl.pallas_call(
        functools.partial(ragged_attention, block),
        out_shape=jax.ShapeDtypeStruct((rollouts, heads, width), jnp.bfloat16),
        in_specs=[pl.BlockSpec(memory_space=pltpu.SMEM), whole, whole, whole, away, away],
        out_specs=whole,
        scratch_shapes=[
            buffers,
            buffers,
            pltpu.SemaphoreType.DMA((3,)),
            pltpu.SemaphoreType.DMA((3,)),
            VMEM((heads, 128), jnp.float32),
            VMEM((heads, 128), jnp.float32),
            VMEM((heads, width), jnp.float32),
        ],
        compiler_params=pltpu.CompilerParams(vmem_limit_bytes=24 * 1024 * 1024),
    )(
        lengths,
        queries.astype(jnp.float32),
        new_keys.astype(jnp.float32),
        new_values.astype(jnp.float32),
        key_cache,
        value_cache,
    )


def shards(
    hidden,
    attention_gain,
    query_weight,
    key_weight,
    value_weight,
    output_weight,
    key_cache,
    value_cache,
    lengths,
    finished,
    feed_gain,
    gate_weight,
    up_weight,
    down_weight,
    final_gain,
    vocab_weight,
    next_tokens,
):
    local_rows = hidden.shape[0]
    key_heads = key_cache.shape[1]
    head_width = key_cache.shape[3]
    groups = H // KVH
    normed = rms_norm(hidden, attention_gain)
    queries = jnp.dot(normed, query_weight, preferred_element_type=jnp.float32).reshape(
        local_rows, key_heads * groups, head_width
    )
    queries = rotate(queries, lengths).astype(jnp.bfloat16)
    new_keys = jnp.dot(normed, key_weight, preferred_element_type=jnp.float32).reshape(
        local_rows, key_heads, head_width
    )
    new_keys = rotate(new_keys, lengths).astype(jnp.bfloat16)
    new_values = (
        jnp.dot(normed, value_weight, preferred_element_type=jnp.float32)
        .astype(jnp.bfloat16)
        .reshape(local_rows, key_heads, head_width)
    )
    attended = cached_attention(
        queries, new_keys, new_values, key_cache, value_cache, lengths
    )
    partial_heads = jnp.dot(
        attended.reshape(local_rows, key_heads * groups * head_width),
        output_weight,
        preferred_element_type=jnp.float32,
    )
    n_dp, n_mp = lax.axis_size("dp"), lax.axis_size("mp")
    width = hidden.shape[1]
    row_type = jax.ShapeDtypeStruct((local_rows, width), jnp.bfloat16)
    all_rows = jax.ShapeDtypeStruct((n_dp, local_rows, width), jnp.bfloat16)
    landing = VMEM((max(n_mp - 1, 1), local_rows, width), jnp.bfloat16)
    feed_in, mixed_hidden = comm_call(
        functools.partial(after_attention, n_dp, n_mp),
        (partial_heads.astype(jnp.bfloat16), hidden, feed_gain[None]),
        (all_rows, row_type),
        [landing] + pairs(n_mp - 1) + pairs(n_dp - 1),
        1,
    )
    feed_in = feed_in.reshape(n_dp * local_rows, width)
    gate = jnp.dot(feed_in, gate_weight, preferred_element_type=jnp.float32)
    upward = jnp.dot(feed_in, up_weight, preferred_element_type=jnp.float32)
    activation = (jax.nn.silu(gate) * upward).astype(jnp.bfloat16)
    partial_feed = jnp.dot(activation, down_weight, preferred_element_type=jnp.float32)
    final = comm_call(
        functools.partial(after_feed, n_dp, n_mp),
        (
            partial_feed.astype(jnp.bfloat16).reshape(n_dp, local_rows, width),
            mixed_hidden,
            final_gain[None],
        ),
        all_rows,
        [
            VMEM((n_dp - 1, local_rows, width), jnp.bfloat16),
            VMEM((local_rows, width), jnp.bfloat16),
            landing,
        ]
        + pairs(n_dp - 1)
        + pairs(n_mp - 1)
        + pairs(n_dp - 1),
        2,
    )
    final = final.reshape(n_dp * local_rows, width)
    logits = jnp.dot(final, vocab_weight, preferred_element_type=jnp.float32)
    vocab_local = vocab_weight.shape[1]
    vocab_start = (lax.axis_index("dp") * n_mp + lax.axis_index("mp")) * vocab_local
    offsets = next_tokens - vocab_start
    matches = lax.broadcasted_iota(jnp.int32, (1, vocab_local), 1) == offsets[:, None]
    picked = jnp.sum(jnp.where(matches, logits, 0.0), axis=-1)
    local_top = jnp.max(logits, axis=-1)
    local_spread = jnp.sum(jnp.exp(logits - local_top[:, None]), axis=-1)
    rollouts = next_tokens.shape[0]
    lanes = -(-rollouts // 128) * 128
    stats = jnp.pad(
        jnp.stack([local_top, local_spread, picked]), ((0, 5), (0, lanes - rollouts))
    )
    chosen = comm_call(
        functools.partial(after_logits, n_dp, n_mp),
        (stats,),
        jax.ShapeDtypeStruct((8, lanes), jnp.float32),
        [
            VMEM((max(n_mp - 1, 1), 8, lanes), jnp.float32),
            VMEM((8, lanes), jnp.float32),
            VMEM((n_dp - 1, 8, lanes), jnp.float32),
        ]
        + pairs(n_mp - 1)
        + pairs(n_dp - 1),
        3,
    )
    chosen = lax.dynamic_slice_in_dim(chosen[0], lax.axis_index("dp") * local_rows, local_rows, 0)
    return jnp.where(finished != 0, 0.0, chosen).astype(jnp.float32)


def solution(mesh):
    in_specs = (
        P("dp", None),
        P(),
        P(None, "mp"),
        P(None, "mp"),
        P(None, "mp"),
        P("mp", None),
        P("dp", "mp", None, None),
        P("dp", "mp", None, None),
        P("dp"),
        P("dp"),
        P(),
        P(None, ("dp", "mp")),
        P(None, ("dp", "mp")),
        P(("dp", "mp"), None),
        P(),
        P(None, ("dp", "mp")),
        P(),
    )
    out_specs = P("dp")
    return jax.shard_map(shards, mesh=mesh, in_specs=in_specs, out_specs=out_specs, check_vma=False)
```

```python
import functools
import math

import jax
import jax.numpy as jnp
from jax import lax
from jax.experimental import pallas as pl
from jax.experimental.pallas import tpu as pltpu
from jax.sharding import PartitionSpec as P

H = 32
KVH = 8


EPSILON = 1e-05
THETA = 500000.0
NEGATIVE = -1e30


def rms_norm(hidden, gain):
    wide = hidden.astype(jnp.float32)
    scale = lax.rsqrt(jnp.mean(wide * wide, axis=-1, keepdims=True) + EPSILON)
    return (wide * scale * gain).astype(jnp.bfloat16)


def rotate(heads, positions):
    half = heads.shape[-1] // 2
    exponent = jnp.arange(half, dtype=jnp.float32) * (-2.0 / heads.shape[-1])
    frequency = jnp.power(jnp.float32(THETA), exponent)
    angles = positions.astype(jnp.float32)[:, None, None] * frequency[None, None, :]
    cosine = jnp.cos(angles)
    sine = jnp.sin(angles)
    former = heads[..., :half]
    latter = heads[..., half:]
    return jnp.concatenate(
        [former * cosine - latter * sine, latter * cosine + former * sine], axis=-1
    )


MESH = pl.DeviceIdType.MESH
VMEM = pltpu.VMEM


def greet(n_dp, n_mp):
    dp, mp = lax.axis_index("dp"), lax.axis_index("mp")
    barrier = pltpu.get_barrier_semaphore()
    for step in range(1, n_mp):
        pl.semaphore_signal(
            barrier, inc=1, device_id=(dp, lax.rem(mp + step, n_mp)), device_id_type=MESH
        )
    for step in range(1, n_dp):
        pl.semaphore_signal(
            barrier, inc=1, device_id=(lax.rem(dp + step, n_dp), mp), device_id_type=MESH
        )
    pl.semaphore_wait(barrier, n_mp + n_dp - 2)
    return dp, mp


def exchange(sources, targets, sends, receives, peers):
    copies = []
    for step, (source, target, peer) in enumerate(zip(sources, targets, peers)):
        copy = pltpu.make_async_remote_copy(
            src_ref=source,
            dst_ref=target,
            send_sem=sends.at[step],
            recv_sem=receives.at[step],
            device_id=peer,
            device_id_type=MESH,
        )
        copy.start()
        copies.append(copy)
    return copies


def across_mp(dp, mp, n_mp):
    return [(dp, lax.rem(mp + step, n_mp)) for step in range(1, n_mp)]


def across_dp(dp, mp, n_dp):
    return [(lax.rem(dp + step, n_dp), mp) for step in range(1, n_dp)]


def normalized(wide, gain):
    scale = lax.rsqrt(jnp.mean(wide * wide, axis=-1, keepdims=True) + EPSILON)
    return (wide * scale * gain).astype(jnp.bfloat16)


def spread_rows(gathered_ref, dp, mp, n_dp, sends, receives):
    mine = gathered_ref.at[dp]
    if n_dp % 2 == 1 or n_dp == 2:
        copies = exchange(
            [mine] * (n_dp - 1),
            [mine] * (n_dp - 1),
            sends,
            receives,
            across_dp(dp, mp, n_dp),
        )
        for copy in copies:
            copy.wait()
        return
    half = n_dp // 2
    twin = (dp + 1 - 2 * lax.rem(dp, 2), mp)
    peers = [(lax.rem(dp + 2 * step, n_dp), mp) for step in range(1, half)]
    copies = exchange([mine] * half, [mine] * half, sends, receives, peers + [twin])
    for step in range(1, half):
        copies[step - 1].wait_recv()
        rows = gathered_ref.at[lax.rem(dp - 2 * step + n_dp, n_dp)]
        forward = pltpu.make_async_remote_copy(
            src_ref=rows,
            dst_ref=rows,
            send_sem=sends.at[half - 1 + step],
            recv_sem=receives.at[half - 1 + step],
            device_id=twin,
            device_id_type=MESH,
        )
        forward.start()
        copies.append(forward)
    for place, copy in enumerate(copies):
        copy.wait_send()
        if place >= half - 1:
            copy.wait_recv()


def after_attention(
    n_dp, n_mp, partial_ref, hidden_ref, gain_ref, gathered_ref, mixed_ref,
    landed, mp_send, mp_receive, dp_send, dp_receive,
):
    dp, mp = greet(n_dp, n_mp)
    copies = exchange(
        [partial_ref] * (n_mp - 1),
        [landed.at[step] for step in range(n_mp - 1)],
        mp_send,
        mp_receive,
        across_mp(dp, mp, n_mp),
    )
    total = partial_ref[...].astype(jnp.float32)
    for step, copy in enumerate(copies):
        copy.wait()
        total = total + landed[step].astype(jnp.float32)
    mixed = (hidden_ref[...].astype(jnp.float32) + total).astype(jnp.bfloat16)
    mixed_ref[...] = mixed
    gathered_ref[dp] = normalized(mixed.astype(jnp.float32), gain_ref[...])
    spread_rows(gathered_ref, dp, mp, n_dp, dp_send, dp_receive)


def after_feed(
    n_dp, n_mp, partial_ref, mixed_ref, gain_ref, gathered_ref,
    arrived, summed, landed, rs_send, rs_receive, mp_send, mp_receive, dp_send, dp_receive,
):
    dp, mp = greet(n_dp, n_mp)
    copies = exchange(
        [partial_ref.at[lax.rem(dp + step, n_dp)] for step in range(1, n_dp)],
        [arrived.at[step] for step in range(n_dp - 1)],
        rs_send,
        rs_receive,
        across_dp(dp, mp, n_dp),
    )
    total = partial_ref[dp].astype(jnp.float32)
    for step, copy in enumerate(copies):
        copy.wait()
        total = total + arrived[step].astype(jnp.float32)
    summed[...] = total.astype(jnp.bfloat16)
    copies = exchange(
        [summed] * (n_mp - 1),
        [landed.at[step] for step in range(n_mp - 1)],
        mp_send,
        mp_receive,
        across_mp(dp, mp, n_mp),
    )
    total = summed[...].astype(jnp.float32)
    for step, copy in enumerate(copies):
        copy.wait()
        total = total + landed[step].astype(jnp.float32)
    residual = (mixed_ref[...].astype(jnp.float32) + total).astype(jnp.bfloat16)
    gathered_ref[dp] = normalized(residual.astype(jnp.float32), gain_ref[...])
    spread_rows(gathered_ref, dp, mp, n_dp, dp_send, dp_receive)


def joined_stats(pieces):
    highest = pieces[0][0:1]
    for piece in pieces[1:]:
        highest = jnp.maximum(highest, piece[0:1])
    spread = sum(piece[1:2] * jnp.exp(piece[0:1] - highest) for piece in pieces)
    picked = sum(piece[2:3] for piece in pieces)
    return highest, spread, picked


def after_logits(
    n_dp, n_mp, stats_ref, out_ref,
    landed, joint, arrived, mp_send, mp_receive, dp_send, dp_receive,
):
    dp, mp = greet(n_dp, n_mp)
    copies = exchange(
        [stats_ref] * (n_mp - 1),
        [landed.at[step] for step in range(n_mp - 1)],
        mp_send,
        mp_receive,
        across_mp(dp, mp, n_mp),
    )
    for copy in copies:
        copy.wait()
    highest, spread, picked = joined_stats(
        [stats_ref[...]] + [landed[step] for step in range(n_mp - 1)]
    )
    joint[...] = jnp.zeros_like(joint)
    joint[0:1] = highest
    joint[1:2] = spread
    joint[2:3] = picked
    copies = exchange(
        [joint] * (n_dp - 1),
        [arrived.at[step] for step in range(n_dp - 1)],
        dp_send,
        dp_receive,
        across_dp(dp, mp, n_dp),
    )
    for copy in copies:
        copy.wait()
    highest, spread, picked = joined_stats(
        [joint[...]] + [arrived[step] for step in range(n_dp - 1)]
    )
    result = picked - (highest + jnp.log(spread))
    out_ref[...] = jnp.broadcast_to(result, out_ref.shape)


def pairs(count):
    return [pltpu.SemaphoreType.DMA((max(count, 1),))] * 2


def comm_call(kernel, operands, out_shape, scratch, number):
    return pl.pallas_call(
        kernel,
        out_shape=out_shape,
        in_specs=[pl.BlockSpec(memory_space=VMEM)] * len(operands),
        out_specs=jax.tree.map(lambda _: pl.BlockSpec(memory_space=VMEM), out_shape),
        scratch_shapes=scratch,
        compiler_params=pltpu.CompilerParams(
            collective_id=number, has_side_effects=True, vmem_limit_bytes=8 * 1024 * 1024
        ),
    )(*operands)


def ragged_attention(
    block, lengths_ref, query_ref, key_ref, value_ref, key_hbm, value_hbm, out_ref,
    keys, values, key_sem, value_sem, tops, totals, sums,
):
    rollouts, heads, width = query_ref.shape
    key_heads = key_ref.shape[1]
    groups = heads // key_heads
    depth = keys.shape[0]
    scale = 1.0 / math.sqrt(width)
    owner = lax.broadcasted_iota(jnp.int32, (heads, 1), 0) // groups

    def by_head(pieces):
        joint = pieces[0]
        for head in range(1, key_heads):
            joint = jnp.where(owner == head, pieces[head], joint)
        return joint

    def blocks_of(row):
        return lax.div(lengths_ref[jnp.minimum(row, rollouts - 1)] + (block - 1), block)

    def following(row, part):
        last = part + 1 >= blocks_of(row)
        return jnp.where(last, row + 1, row), jnp.where(last, 0, part + 1)

    def copies(slot, row, part):
        places = pl.ds(pl.multiple_of(part * block, block), block)
        return (
            pltpu.make_async_copy(
                key_hbm.at[row, :, places, :], keys.at[slot], key_sem.at[slot]
            ),
            pltpu.make_async_copy(
                value_hbm.at[row, :, places, :], values.at[slot], value_sem.at[slot]
            ),
        )

    def fetch(slot, row, part):
        for copy in copies(slot, row, part):
            copy.start()

    steps = sum(blocks_of(row) for row in range(rollouts))
    ahead = (jnp.int32(0), jnp.int32(0))
    for slot in range(depth - 1):
        def begin(slot=slot, ahead=ahead):
            fetch(slot, *ahead)

        pl.when(slot < steps)(begin)
        ahead = following(*ahead)

    def step_body(step, carry):
        row, part, ahead_row, ahead_part = carry
        slot = lax.rem(step, depth)

        @pl.when(step + (depth - 1) < steps)
        def _():
            fetch(lax.rem(step + (depth - 1), depth), ahead_row, ahead_part)

        query = query_ref[row]

        @pl.when(part == 0)
        def _():
            own_key = by_head([key_ref[row, head : head + 1] for head in range(key_heads)])
            own_value = by_head([value_ref[row, head : head + 1] for head in range(key_heads)])
            own = jnp.sum(query * own_key, axis=-1, keepdims=True) * scale
            tops[...] = jnp.broadcast_to(own, tops.shape)
            totals[...] = jnp.ones_like(totals)
            sums[...] = jnp.broadcast_to(own_value, sums.shape)

        key_copy, value_copy = copies(slot, row, part)
        key_copy.wait()
        narrow = query.astype(jnp.bfloat16)
        scores = by_head(
            [
                lax.dot_general(
                    narrow,
                    keys[slot, head],
                    (((1,), (1,)), ((), ())),
                    preferred_element_type=jnp.float32,
                )
                for head in range(key_heads)
            ]
        )
        places = part * block + lax.broadcasted_iota(jnp.int32, (1, block), 1)
        scores = jnp.where(places < lengths_ref[row], scores * scale, NEGATIVE)
        former = tops[:, 0:1]
        top = jnp.maximum(former, jnp.max(scores, axis=-1, keepdims=True))
        fade = jnp.exp(former - top)
        weights = jnp.exp(scores - top)
        total = totals[:, 0:1] * fade + jnp.sum(weights, axis=-1, keepdims=True)
        rounded = weights.astype(jnp.bfloat16)
        value_copy.wait()
        mixed = by_head(
            [
                jnp.dot(rounded, values[slot, head], preferred_element_type=jnp.float32)
                for head in range(key_heads)
            ]
        )
        mixed = sums[...] * fade + mixed
        tops[...] = jnp.broadcast_to(top, tops.shape)
        totals[...] = jnp.broadcast_to(total, totals.shape)
        sums[...] = mixed
        out_ref[row] = (mixed / total).astype(jnp.bfloat16)
        return following(row, part) + following(ahead_row, ahead_part)

    lax.fori_loop(0, steps, step_body, (jnp.int32(0), jnp.int32(0)) + ahead)


def cached_attention(queries, new_keys, new_values, key_cache, value_cache, lengths):
    rollouts, key_heads, places, width = key_cache.shape
    heads = queries.shape[1]
    block = math.gcd(places, 2048)
    buffers = VMEM((3, key_heads, block, width), jnp.bfloat16)
    whole = pl.BlockSpec(memory_space=VMEM)
    away = pl.BlockSpec(memory_space=pltpu.HBM)
    return pl.pallas_call(
        functools.partial(ragged_attention, block),
        out_shape=jax.ShapeDtypeStruct((rollouts, heads, width), jnp.bfloat16),
        in_specs=[pl.BlockSpec(memory_space=pltpu.SMEM), whole, whole, whole, away, away],
        out_specs=whole,
        scratch_shapes=[
            buffers,
            buffers,
            pltpu.SemaphoreType.DMA((3,)),
            pltpu.SemaphoreType.DMA((3,)),
            VMEM((heads, 128), jnp.float32),
            VMEM((heads, 128), jnp.float32),
            VMEM((heads, width), jnp.float32),
        ],
        compiler_params=pltpu.CompilerParams(vmem_limit_bytes=50 * 1024 * 1024),
        cost_estimate=pl.CostEstimate(
            flops=10_000_000_000, bytes_accessed=20_000_000, transcendentals=0
        ),
    )(
        lengths,
        queries.astype(jnp.float32),
        new_keys.astype(jnp.float32),
        new_values.astype(jnp.float32),
        key_cache,
        value_cache,
    )


def shards(
    hidden,
    attention_gain,
    query_weight,
    key_weight,
    value_weight,
    output_weight,
    key_cache,
    value_cache,
    lengths,
    finished,
    feed_gain,
    gate_weight,
    up_weight,
    down_weight,
    final_gain,
    vocab_weight,
    next_tokens,
):
    local_rows = hidden.shape[0]
    key_heads = key_cache.shape[1]
    head_width = key_cache.shape[3]
    groups = H // KVH
    normed = rms_norm(hidden, attention_gain)
    queries = jnp.dot(normed, query_weight, preferred_element_type=jnp.float32).reshape(
        local_rows, key_heads * groups, head_width
    )
    queries = rotate(queries, lengths).astype(jnp.bfloat16)
    new_keys = jnp.dot(normed, key_weight, preferred_element_type=jnp.float32).reshape(
        local_rows, key_heads, head_width
    )
    new_keys = rotate(new_keys, lengths).astype(jnp.bfloat16)
    new_values = (
        jnp.dot(normed, value_weight, preferred_element_type=jnp.float32)
        .astype(jnp.bfloat16)
        .reshape(local_rows, key_heads, head_width)
    )
    attended = cached_attention(
        queries, new_keys, new_values, key_cache, value_cache, lengths
    )
    partial_heads = jnp.dot(
        attended.reshape(local_rows, key_heads * groups * head_width),
        output_weight,
        preferred_element_type=jnp.float32,
    )
    n_dp, n_mp = lax.axis_size("dp"), lax.axis_size("mp")
    width = hidden.shape[1]
    row_type = jax.ShapeDtypeStruct((local_rows, width), jnp.bfloat16)
    all_rows = jax.ShapeDtypeStruct((n_dp, local_rows, width), jnp.bfloat16)
    landing = VMEM((max(n_mp - 1, 1), local_rows, width), jnp.bfloat16)
    feed_in, mixed_hidden = comm_call(
        functools.partial(after_attention, n_dp, n_mp),
        (partial_heads.astype(jnp.bfloat16), hidden, feed_gain[None]),
        (all_rows, row_type),
        [landing] + pairs(n_mp - 1) + pairs(n_dp - 1),
        1,
    )
    feed_in = feed_in.reshape(n_dp * local_rows, width)
    gate = jnp.dot(feed_in, gate_weight, preferred_element_type=jnp.float32)
    upward = jnp.dot(feed_in, up_weight, preferred_element_type=jnp.float32)
    activation = (jax.nn.silu(gate) * upward).astype(jnp.bfloat16)
    partial_feed = jnp.dot(activation, down_weight, preferred_element_type=jnp.float32)
    final = comm_call(
        functools.partial(after_feed, n_dp, n_mp),
        (
            partial_feed.astype(jnp.bfloat16).reshape(n_dp, local_rows, width),
            mixed_hidden,
            final_gain[None],
        ),
        all_rows,
        [
            VMEM((n_dp - 1, local_rows, width), jnp.bfloat16),
            VMEM((local_rows, width), jnp.bfloat16),
            landing,
        ]
        + pairs(n_dp - 1)
        + pairs(n_mp - 1)
        + pairs(n_dp - 1),
        2,
    )
    final = final.reshape(n_dp * local_rows, width)
    logits = jnp.dot(final, vocab_weight, preferred_element_type=jnp.float32)
    vocab_local = vocab_weight.shape[1]
    vocab_start = (lax.axis_index("dp") * n_mp + lax.axis_index("mp")) * vocab_local
    offsets = next_tokens - vocab_start
    matches = lax.broadcasted_iota(jnp.int32, (1, vocab_local), 1) == offsets[:, None]
    picked = jnp.sum(jnp.where(matches, logits, 0.0), axis=-1)
    local_top = jnp.max(logits, axis=-1)
    local_spread = jnp.sum(jnp.exp(logits - local_top[:, None]), axis=-1)
    rollouts = next_tokens.shape[0]
    lanes = -(-rollouts // 128) * 128
    stats = jnp.pad(
        jnp.stack([local_top, local_spread, picked]), ((0, 5), (0, lanes - rollouts))
    )
    chosen = comm_call(
        functools.partial(after_logits, n_dp, n_mp),
        (stats,),
        jax.ShapeDtypeStruct((8, lanes), jnp.float32),
        [
            VMEM((max(n_mp - 1, 1), 8, lanes), jnp.float32),
            VMEM((8, lanes), jnp.float32),
            VMEM((n_dp - 1, 8, lanes), jnp.float32),
        ]
        + pairs(n_mp - 1)
        + pairs(n_dp - 1),
        3,
    )
    chosen = lax.dynamic_slice_in_dim(chosen[0], lax.axis_index("dp") * local_rows, local_rows, 0)
    return jnp.where(finished != 0, 0.0, chosen).astype(jnp.float32)


def solution(mesh):
    in_specs = (
        P("dp", None),
        P(),
        P(None, "mp"),
        P(None, "mp"),
        P(None, "mp"),
        P("mp", None),
        P("dp", "mp", None, None),
        P("dp", "mp", None, None),
        P("dp"),
        P("dp"),
        P(),
        P(None, ("dp", "mp")),
        P(None, ("dp", "mp")),
        P(("dp", "mp"), None),
        P(),
        P(None, ("dp", "mp")),
        P(),
    )
    out_specs = P("dp")
    return jax.shard_map(shards, mesh=mesh, in_specs=in_specs, out_specs=out_specs, check_vma=False)
```
